128 devices in a mesh: atom: 32 (over x, z, core), energy: 4 (over y).
Axes of the slice: x: 4, y: 4, z: 4, core: 2. Of those that a mesh axis runs over, the one named last changes fastest.
Arguments:
- t_matrix: float32 [4, 256, 16, 16], P('energy', 'atom'), may hold values from -1.5 to 1.5
- structure: bfloat16 [4, 256, 1024, 1024], P('energy', 'atom'), may hold values from -0.125 to 0.125
- radial: bfloat16 [4, 256, 16, 1024], P('energy', 'atom'), may hold values from -3 to 3
- weights: float32 [4], P('energy'), may hold values from 0.1 to 1
- neighbours: int32 [256, 64], P('atom'), may hold values from 0 to 255, as said below
- live: int32 [256, 64], P('atom'), may hold values from 0 to 1, as said below
Outputs:
- density: float32 [256, 1024], P('atom', 'energy')
The draws below stay inside these ranges and needn't reach their ends.
Inputs may be any that keep to these rules, and one draw needn't show every extreme that they name: `neighbours`: slot 0 of atom i holds i itself. Atom i lies at index i // 8 of the atom axis, and every neighbour of it lies at an index that differs from that one by at most 3 around the axis, which closes into a loop; both extremes occur in every draw. An atom may appear in several slots of one zone. `live`: each row is 1 on its first slots and 0 after; slot 0 is always 1, at least 16 slots are 1, and some atom has all 64 slots 1.
All inputs are finite; a program needn't handle non-finite values.
Results may differ from the reference program's by a relative error of at most 0.0043.
Values sent between devices are 32-bit elements; how exact they have to be, the bound alone decides.
A program may use at most 128 MiB of HBM per device.

```python
import math
import jax
import jax.numpy as jnp
from jax import lax

LM = 16
NB = 64
R = 1024
ITERS = 4
SPAN = 3
A_DEV = 8
ATOMS = 256
ENERGIES = 4


def draw_neighbours(key, part):
    first_key, second_key = jax.random.split(jax.random.fold_in(key, 11))
    n_devices = ATOMS // A_DEV
    owner = jnp.arange(ATOMS, dtype=jnp.int32) // A_DEV
    offsets = jax.random.randint(first_key, (ATOMS, NB), -SPAN, SPAN + 1)
    offsets = offsets.at[:, 1].set(SPAN).at[:, 2].set(-SPAN)
    slots = jax.random.randint(second_key, (ATOMS, NB), 0, A_DEV)
    device = (owner[:, None] + offsets + n_devices) % n_devices
    picked = device * A_DEV + slots
    picked = picked.at[:, 0].set(jnp.arange(ATOMS, dtype=jnp.int32))
    return picked.astype(jnp.int32)


def draw_live(key, part):
    counts = jax.random.randint(jax.random.fold_in(key, 23), (ATOMS,), NB // 4, NB + 1)
    counts = counts.at[0].set(NB)
    return (jnp.arange(NB)[None, :] < counts[:, None]).astype(jnp.int32)


def block_levels(rng, shape, pieces, smallest, top_value):
    gain, own = 1.0, jax.random.fold_in(rng, 6)
    for axis_at, blocks in pieces:
        draws = jnp.exp(jax.random.uniform(jax.random.fold_in(own, axis_at), (blocks,), jnp.float32, smallest / len(pieces), top_value / len(pieces)))
        gain = gain * jnp.repeat(draws, shape[axis_at] // blocks).reshape([-1 if axis == axis_at else 1 for axis in range(len(shape))])
    return gain


def bell_draw(key, shape, deviation, most, cuts=(), kind=jnp.bfloat16):
    loudness = block_levels(key, shape, cuts, -0.22, 0.18) if cuts else 1.0
    drawn = jax.random.normal(key, shape, jnp.float32) * deviation * loudness
    return jnp.minimum(jnp.maximum(drawn, -most), most).astype(kind)


def setup_inputs(seed: int = 0) -> dict:
    splits = jax.random.split(jax.random.key(seed), 7)
    return {
        "t_matrix": bell_draw(splits[0], (ENERGIES, ATOMS, LM, LM), LM ** -0.5, 1.5, ((0, 4), (1, 32)), jnp.float32),
        "structure": bell_draw(splits[1], (ENERGIES, ATOMS, NB * LM, NB * LM), (2 * NB * LM) ** -0.5, 0.125, ((0, 4), (1, 32))),
        "radial": bell_draw(splits[2], (ENERGIES, ATOMS, LM, R), 0.5, 3.0, ((0, 4), (1, 32))),
        "weights": jnp.clip(jnp.exp(math.log(1.0) - 2.3025851 * jax.random.uniform(splits[3], (ENERGIES,), jnp.float32) ** block_levels(splits[3], (ENERGIES,), ((0, 4),), -0.2, 0.2)), 0.1, 1.0),
        "neighbours": draw_neighbours(jax.random.fold_in(splits[6], 71), 0),
        "live": draw_live(jax.random.fold_in(splits[6], 71), 0),
    }


def zone_column(args):
    t_self, g_here, zt_here = args
    rest = jnp.zeros((NB - 1, LM, LM), jnp.float32)
    first = jnp.concatenate([t_self[None], rest], axis=0)
    g_float = g_here.astype(jnp.float32)
    zt_float = zt_here.astype(jnp.float32)
    column = first
    for step in range(ITERS):
        flat_b = lax.optimization_barrier(column.astype(jnp.bfloat16))
        flat = flat_b.astype(jnp.float32).reshape(NB * LM, LM)
        image = jnp.dot(g_float, flat, precision=lax.Precision.HIGHEST)
        image_b = lax.optimization_barrier(image.astype(jnp.bfloat16))
        image_f = image_b.astype(jnp.float32).reshape(NB, LM, LM)
        column = first + jnp.einsum("sij,sjk->sik", zt_float, image_f, precision=lax.Precision.HIGHEST)
    return column


def reference(t_matrix, structure, radial, weights, neighbours, live):
    live_f = live.astype(jnp.float32)
    flat_ids = neighbours.reshape(-1)

    def per_energy(args):
        t_here, g_here, z_here = args
        zone_t = (t_here[neighbours] * live_f[:, :, None, None]).astype(jnp.bfloat16)
        column = lax.map(zone_column, (t_here, g_here, zone_t))
        blocks = (column * live_f[:, :, None, None]).reshape(ATOMS * NB, LM, LM)
        received = jax.ops.segment_sum(blocks, flat_ids, num_segments=ATOMS)
        received_b = lax.optimization_barrier(received.astype(jnp.bfloat16))
        z_float = z_here.astype(jnp.float32)
        turned = jnp.einsum("alm,amr->alr", received_b.astype(jnp.float32), z_float, precision=lax.Precision.HIGHEST)
        return jnp.sum(z_float * turned, axis=1)

    partial_value = lax.map(per_energy, (t_matrix, structure, radial))
    return jnp.sum(weights[:, None, None] * partial_value, axis=0)
```

```python
import functools

import jax
import jax.numpy as jnp
from jax import lax
from jax.experimental import pallas as pl
from jax.experimental.pallas import tpu as pltpu
from jax.sharding import PartitionSpec as P

MESH = pl.DeviceIdType.MESH
F32 = jnp.float32
BF16 = jnp.bfloat16

SPAN = 3
PLACES = 2 * SPAN + 1
SWEEPS = 4
LM = 16
NB = 64
A_DEV = 8
LANES = 128
SIZE = NB * LM
TILE = 256


def iota(shape, dim):
    return lax.broadcasted_iota(jnp.int32, shape, dim)


def ones_where(cond):
    return jnp.where(cond, 1.0, 0.0).astype(F32)


def kernel(
    n_atom, n_energy,
    t_ref, rad_ref, w_ref, nbr_ref, live_ref, s_hbm, out_ref,
    s_buf, st_buf, q_buf, bd_buf, table, t_self, t_land, first_buf, img_buf, spread_buf, tbx_buf, t_tiled,
    g_send, g_land, p_send, p_land, slot_of,
    s_sem, t_send_sem, t_recv_sem, g_send_sem, g_recv_sem, p_send_sem, p_recv_sem,
):
    me = lax.axis_index("atom")
    mine = lax.axis_index("energy")

    def atom_at(by):
        return lax.rem(me + by + n_atom, n_atom)

    def energy_at(by):
        return lax.rem(mine + by, n_energy)

    others = [place for place in range(PLACES) if place != SPAN]

    def s_copy(a):
        return pltpu.make_async_copy(s_hbm.at[a], s_buf.at[a], s_sem.at[a])

    for a in range(A_DEV):
        s_copy(a).start()

    barrier = pltpu.get_barrier_semaphore()
    for place in others:
        pl.semaphore_signal(barrier, inc=1, device_id={"atom": atom_at(place - SPAN)}, device_id_type=MESH)
    for by in range(1, n_energy):
        pl.semaphore_signal(barrier, inc=1, device_id={"energy": energy_at(by)}, device_id_type=MESH)

    t_rows = t_ref[...]
    t_wide = jnp.concatenate([t_rows, jnp.zeros((A_DEV * LM, LANES - LM), F32)], axis=1)
    t_turned = t_wide.T[0:LM, :]
    t_self[...] = t_turned
    lane16 = iota((LM, LANES), 1)
    for a in range(A_DEV):
        moved = t_turned if a == 0 else pltpu.roll(t_turned, LANES - a * LM, 1)
        first_buf[a] = jnp.where(lane16 < LM, moved, 0.0)

    pl.semaphore_wait(barrier, len(others) + n_energy - 1)

    def t_copy(place):
        return pltpu.make_async_remote_copy(
            src_ref=t_self, dst_ref=t_land.at[2 * SPAN - place],
            send_sem=t_send_sem.at[place], recv_sem=t_recv_sem.at[2 * SPAN - place],
            device_id={"atom": atom_at(place - SPAN)}, device_id_type=MESH,
        )

    for place in others:
        t_copy(place).start()

    lane = iota((LANES, LANES), 1)
    row = iota((LANES, LANES), 0)
    t_b = t_rows.astype(BF16)
    expand = ones_where(iota((LM, LANES), 1) // A_DEV == iota((LM, LANES), 0)).astype(BF16)
    tbx = jnp.dot(t_b, expand, preferred_element_type=F32)
    tbx = jnp.where(lane % A_DEV == row // LM, tbx, 0.0).astype(BF16)
    tbx_buf[:, 0:LANES] = tbx
    tbx_buf[:, LANES:] = tbx
    tiled = t_wide
    for by in (16, 32, 64):
        tiled = tiled + pltpu.roll(tiled, by, 1)
    t_tiled[...] = tiled
    for a in range(A_DEV):
        spread_buf[:, a * LANES:(a + 1) * LANES] = ones_where(
            (row // LM == a) & (row % LM == lane % LM)
        ).astype(BF16)

    where_to = lane16 - A_DEV * (iota((LM, LANES), 0) % 2)

    def hot(step, carry):
        a = step // (NB // 8)
        for k in range(8):
            s = (step % (NB // 8)) * 8 + k
            nbr = nbr_ref[a, s]
            alive = live_ref[a, s]
            place = lax.rem(nbr // A_DEV - me + SPAN + n_atom, n_atom)
            inner = lax.rem(nbr, A_DEV)
            base = alive * (place * LM + inner + 1) - 1
            slot_of[a, s] = alive * (place * A_DEV + inner - PLACES * A_DEV) + PLACES * A_DEV
            q_buf[a, pl.ds(pl.multiple_of(s * LM, LM), LM), :] = jnp.where(
                (where_to == base) & (base >= 0), 1.0, 0.0
            ).astype(BF16)
        return carry

    lax.fori_loop(0, A_DEV * NB // 8, hot, 0)

    def turn(a, carry):
        s_copy(a).wait()
        for bi in range(SIZE // TILE):
            for bj in range(SIZE // TILE):
                st_buf[a, bj * TILE:(bj + 1) * TILE, bi * TILE:(bi + 1) * TILE] = s_buf[
                    a, bi * TILE:(bi + 1) * TILE, bj * TILE:(bj + 1) * TILE
                ].T
        img_buf[a] = jnp.dot(
            first_buf[a].astype(BF16), st_buf[a, 0:LANES, :], preferred_element_type=F32
        ).astype(BF16)
        return carry

    lax.fori_loop(0, A_DEV, turn, 0)

    t_land[SPAN] = t_self[...]
    for place in others:
        t_copy(place).wait_send()
        t_copy(2 * SPAN - place).wait_recv()
    landed = t_land[...].reshape(PLACES * LM, LANES).astype(BF16)
    wide = jnp.dot(landed, spread_buf[...], preferred_element_type=F32).astype(BF16)
    for place in range(PLACES):
        for a in range(A_DEV):
            table[place * A_DEV + a] = wide[place * LM:(place + 1) * LM, a * LANES:(a + 1) * LANES]
    table[PLACES * A_DEV] = jnp.zeros((LM, LANES), BF16)

    keep = [ones_where(lane16 // LM == r).astype(BF16) for r in range(8)]

    def zone_blocks(a):
        for g in range(4):
            for h in range(2):
                for r in range(8):
                    s = g * 16 + h * 8 + r
                    bd_buf[a, g, r * LM:(r + 1) * LM, h * LANES:(h + 1) * LANES] = (
                        table[slot_of[a, s]] * keep[r]
                    )

    def zone(a):
        image = img_buf[a]
        parts = []
        for g in range(4):
            pair = jnp.concatenate(
                [image[:, 2 * g * LANES:(2 * g + 1) * LANES], image[:, (2 * g + 1) * LANES:(2 * g + 2) * LANES]],
                axis=0,
            )
            both = jnp.dot(pair, bd_buf[a, g], preferred_element_type=F32)
            parts.append(both[0:LM, 0:LANES])
            parts.append(both[LM:2 * LM, LANES:])
        parts[0] = parts[0] + first_buf[a]
        return jnp.concatenate([part.astype(BF16) for part in parts], axis=1)

    def sweep(a, flat):
        img_buf[a] = jnp.dot(flat, st_buf[a], preferred_element_type=F32).astype(BF16)

    for a in range(A_DEV):
        zone_blocks(a)
    for step in range(SWEEPS - 1):
        for a in range(A_DEV):
            sweep(a, zone(a))

    total = jnp.zeros((LANES, LANES), F32)
    pick = [ones_where((lane16 % LM) // 2 == h).astype(BF16) for h in range(8)]
    for a in range(A_DEV):
        image = img_buf[a]
        rows = jnp.concatenate([image * jnp.concatenate([pick[h]] * 8, axis=1) for h in range(8)], axis=0)
        total = total + jnp.dot(rows, q_buf[a], preferred_element_type=F32)
    g_send[...] = total.T

    def g_copy(place):
        return pltpu.make_async_remote_copy(
            src_ref=g_send.at[pl.ds(place * LM, LM)], dst_ref=g_land.at[2 * SPAN - place],
            send_sem=g_send_sem.at[place], recv_sem=g_recv_sem.at[2 * SPAN - place],
            device_id={"atom": atom_at(place - SPAN)}, device_id_type=MESH,
        )

    for place in others:
        g_copy(place).start()
    owned = g_send[SPAN * LM:(SPAN + 1) * LM, :]
    for place in others:
        g_copy(2 * SPAN - place).wait_recv()
        owned = owned + g_land[place]

    high = owned.astype(BF16)
    low = (owned - high.astype(F32)).astype(BF16)
    apart = ones_where(row // LM == lane // LM).astype(BF16)
    stacked = jnp.concatenate(
        [jnp.concatenate([high] * 8, axis=0) * apart, jnp.concatenate([low] * 8, axis=0) * apart], axis=0
    )
    received = jnp.dot(tbx_buf[...], stacked, preferred_element_type=F32)
    for by in (16, 32, 64):
        received = received + pltpu.roll(received, by, 1)
    received = received + t_tiled[...]
    received_b = received.astype(BF16) * apart
    radial = rad_ref[...]
    turned = jnp.dot(received_b, radial, preferred_element_type=F32)
    product = radial.astype(F32) * turned
    partial = product.reshape(A_DEV, LM, product.shape[1]).sum(axis=1) * w_ref[0]
    chunk = product.shape[1] // n_energy
    for e in range(n_energy):
        p_send[e] = partial[:, e * chunk:(e + 1) * chunk]

    def p_copy(by):
        return pltpu.make_async_remote_copy(
            src_ref=p_send.at[energy_at(by)], dst_ref=p_land.at[by - 1],
            send_sem=p_send_sem.at[by - 1], recv_sem=p_recv_sem.at[by - 1],
            device_id={"energy": energy_at(by)}, device_id_type=MESH,
        )

    for by in range(1, n_energy):
        p_copy(by).start()
    density = p_send[mine]
    for by in range(1, n_energy):
        p_copy(by).wait_recv()
        density = density + p_land[by - 1]
    out_ref[...] = density
    for place in others:
        g_copy(place).wait_send()
    for by in range(1, n_energy):
        p_copy(by).wait_send()


def shards(n_atom, n_energy, t_matrix, structure, radial, weights, neighbours, live):
    r = radial.shape[-1]
    vmem = pl.BlockSpec(memory_space=pltpu.VMEM)
    smem = pl.BlockSpec(memory_space=pltpu.SMEM)
    return pl.pallas_call(
        functools.partial(kernel, n_atom, n_energy),
        out_shape=jax.ShapeDtypeStruct((A_DEV, r // n_energy), F32),
        in_specs=[vmem, vmem, smem, smem, smem, pl.BlockSpec(memory_space=pl.ANY)],
        out_specs=vmem,
        scratch_shapes=[
            pltpu.VMEM((A_DEV, SIZE, SIZE), BF16),
            pltpu.VMEM((A_DEV, SIZE, SIZE), BF16),
            pltpu.VMEM((A_DEV, SIZE, LANES), BF16),
            pltpu.VMEM((A_DEV, 4, LANES, TILE), BF16),
            pltpu.VMEM((PLACES * A_DEV + 8, LM, LANES), BF16),
            pltpu.VMEM((LM, LANES), F32),
            pltpu.VMEM((PLACES, LM, LANES), F32),
            pltpu.VMEM((A_DEV, LM, LANES), F32),
            pltpu.VMEM((A_DEV, LM, SIZE), BF16),
            pltpu.VMEM((LANES, A_DEV * LANES), BF16),
            pltpu.VMEM((LANES, 2 * LANES), BF16),
            pltpu.VMEM((LANES, LANES), F32),
            pltpu.VMEM((LANES, LANES), F32),
            pltpu.VMEM((PLACES, LM, LANES), F32),
            pltpu.VMEM((n_energy, A_DEV, r // n_energy), F32),
            pltpu.VMEM((n_energy - 1, A_DEV, r // n_energy), F32),
            pltpu.SMEM((A_DEV, NB), jnp.int32),
            pltpu.SemaphoreType.DMA((A_DEV,)),
            pltpu.SemaphoreType.DMA((PLACES,)),
            pltpu.SemaphoreType.DMA((PLACES,)),
            pltpu.SemaphoreType.DMA((PLACES,)),
            pltpu.SemaphoreType.DMA((PLACES,)),
            pltpu.SemaphoreType.DMA((n_energy - 1,)),
            pltpu.SemaphoreType.DMA((n_energy - 1,)),
        ],
        compiler_params=pltpu.CompilerParams(
            collective_id=0, has_side_effects=True, vmem_limit_bytes=60 * 1024 * 1024
        ),
    )(
        t_matrix.reshape(A_DEV * LM, LM),
        radial.reshape(A_DEV * LM, r),
        weights,
        neighbours,
        live,
        structure.reshape(A_DEV, SIZE, SIZE),
    )


def solution(mesh):
    in_specs = (
        P("energy", "atom", None, None),
        P("energy", "atom", None, None),
        P("energy", "atom", None, None),
        P("energy"),
        P("atom", None),
        P("atom", None),
    )
    body = functools.partial(shards, mesh.shape["atom"], mesh.shape["energy"])
    return jax.shard_map(body, mesh=mesh, in_specs=in_specs, out_specs=P("atom", "energy"), check_vma=False)
```

```python
import functools

import jax
import jax.numpy as jnp
from jax import lax
from jax.experimental import pallas as pl
from jax.experimental.pallas import tpu as pltpu
from jax.sharding import PartitionSpec as P

MESH = pl.DeviceIdType.MESH
F32 = jnp.float32
BF16 = jnp.bfloat16

SPAN = 3
PLACES = 2 * SPAN + 1
SWEEPS = 4
LM = 16
NB = 64
A_DEV = 8
LANES = 128
SIZE = NB * LM
TILE = 256
EARLY = 3


def iota(shape, dim):
    return lax.broadcasted_iota(jnp.int32, shape, dim)


def ones_where(cond):
    return jnp.where(cond, 1.0, 0.0).astype(F32)


def kernel(
    n_atom, n_energy,
    t_hbm, rad_hbm, w_ref, nbr_hbm, live_hbm, s_hbm, out_ref,
    t_ref, rad_ref, nbr_ref, live_ref, slot_vec, pattern, s_buf, st_buf, q_buf, bd_buf, table, t_self, t_land, first_buf, img_buf, spread_buf, tbx_buf, t_tiled,
    g_send, g_land, p_send, p_land, slot_of,
    in_sem, s_sem, t_send_sem, t_recv_sem, g_send_sem, g_recv_sem, p_send_sem, p_recv_sem,
):
    me = lax.axis_index("atom")
    mine = lax.axis_index("energy")

    def atom_at(by):
        return lax.rem(me + by + n_atom, n_atom)

    def energy_at(by):
        return lax.rem(mine + by, n_energy)

    others = [place for place in range(PLACES) if place != SPAN]

    t_in = pltpu.make_async_copy(t_hbm, t_ref, in_sem.at[0])
    nbr_in = pltpu.make_async_copy(nbr_hbm, nbr_ref, in_sem.at[1])
    live_in = pltpu.make_async_copy(live_hbm, live_ref, in_sem.at[2])
    rad_in = pltpu.make_async_copy(rad_hbm, rad_ref, in_sem.at[3])
    t_in.start()
    nbr_in.start()
    live_in.start()

    barrier = pltpu.get_barrier_semaphore()
    for place in others:
        pl.semaphore_signal(barrier, inc=1, device_id={"atom": atom_at(place - SPAN)}, device_id_type=MESH)
    for by in range(1, n_energy):
        pl.semaphore_signal(barrier, inc=1, device_id={"energy": energy_at(by)}, device_id_type=MESH)

    def s_copy(a):
        return pltpu.make_async_copy(s_hbm.at[a], s_buf.at[a], s_sem.at[a])

    for a in range(A_DEV):
        s_copy(a).start()
    rad_in.start()

    t_in.wait()
    t_rows = t_ref[...]
    t_wide = jnp.concatenate([t_rows, jnp.zeros((A_DEV * LM, LANES - LM), F32)], axis=1)
    t_turned = t_wide.T[0:LM, :]
    t_self[...] = t_turned
    lane16 = iota((LM, LANES), 1)
    for a in range(A_DEV):
        moved = t_turned if a == 0 else pltpu.roll(t_turned, LANES - a * LM, 1)
        first_buf[a] = jnp.where(lane16 < LM, moved, 0.0)

    nbr_in.wait()
    live_in.wait()
    nbr = nbr_ref[...]
    place = lax.rem(nbr // A_DEV - me + SPAN + n_atom, n_atom)
    slot_vec[...] = jnp.where(live_ref[...] > 0, place * A_DEV + lax.rem(nbr, A_DEV), PLACES * A_DEV)
    slot_out = pltpu.make_async_copy(slot_vec, slot_of, in_sem.at[4])
    slot_out.start()

    def turn(a, carry):
        s_copy(a).wait()
        for bi in range(SIZE // TILE):
            for bj in range(SIZE // TILE):
                st_buf[a, bj * TILE:(bj + 1) * TILE, bi * TILE:(bi + 1) * TILE] = s_buf[
                    a, bi * TILE:(bi + 1) * TILE, bj * TILE:(bj + 1) * TILE
                ].T
        img_buf[a] = jnp.dot(
            first_buf[a].astype(BF16), st_buf[a, 0:LANES, :], preferred_element_type=F32
        ).astype(BF16)
        return carry

    lax.fori_loop(0, EARLY, turn, 0)
    pl.semaphore_wait(barrier, len(others) + n_energy - 1)

    def t_copy(place):
        return pltpu.make_async_remote_copy(
            src_ref=t_self, dst_ref=t_land.at[2 * SPAN - place],
            send_sem=t_send_sem.at[place], recv_sem=t_recv_sem.at[2 * SPAN - place],
            device_id={"atom": atom_at(place - SPAN)}, device_id_type=MESH,
        )

    for place in others:
        t_copy(place).start()

    lane = iota((LANES, LANES), 1)
    row = iota((LANES, LANES), 0)
    t_b = t_rows.astype(BF16)
    expand = ones_where(iota((LM, LANES), 1) // A_DEV == iota((LM, LANES), 0)).astype(BF16)
    tbx = jnp.dot(t_b, expand, preferred_element_type=F32)
    tbx = jnp.where(lane % A_DEV == row // LM, tbx, 0.0).astype(BF16)
    tbx_buf[:, 0:LANES] = tbx
    tbx_buf[:, LANES:] = tbx
    tiled = t_wide
    for by in (16, 32, 64):
        tiled = tiled + pltpu.roll(tiled, by, 1)
    t_tiled[...] = tiled
    for a in range(A_DEV):
        spread_buf[:, a * LANES:(a + 1) * LANES] = ones_where(
            (row // LM == a) & (row % LM == lane % LM)
        ).astype(BF16)

    lax.fori_loop(EARLY, A_DEV, turn, 0)

    where_to = lane16 - A_DEV * (iota((LM, LANES), 0) % 2)
    for place in range(PLACES):
        for a in range(A_DEV):
            pattern[place * A_DEV + a] = ones_where(where_to == place * LM + a).astype(BF16)
    pattern[PLACES * A_DEV] = jnp.zeros((LM, LANES), BF16)
    slot_out.wait()

    def hot(a, carry):
        for s in range(NB):
            q_buf[a, s * LM:(s + 1) * LM, :] = pattern[slot_of[a, s]]
        return carry

    lax.fori_loop(0, A_DEV, hot, 0)

    t_land[SPAN] = t_self[...]
    for place in others:
        t_copy(place).wait_send()
        t_copy(2 * SPAN - place).wait_recv()
    landed = t_land[...].reshape(PLACES * LM, LANES).astype(BF16)
    wide = jnp.dot(landed, spread_buf[...], preferred_element_type=F32).astype(BF16)
    for place in range(PLACES):
        for a in range(A_DEV):
            table[place * A_DEV + a] = wide[place * LM:(place + 1) * LM, a * LANES:(a + 1) * LANES]
    table[PLACES * A_DEV] = jnp.zeros((LM, LANES), BF16)

    keep = [ones_where(lane16 // LM == r).astype(BF16) for r in range(8)]

    def zone_blocks(a):
        for g in range(4):
            for h in range(2):
                for r in range(8):
                    s = g * 16 + h * 8 + r
                    bd_buf[a, g, r * LM:(r + 1) * LM, h * LANES:(h + 1) * LANES] = (
                        table[slot_of[a, s]] * keep[r]
                    )

    def zone(a):
        image = img_buf[a]
        parts = []
        for g in range(4):
            pair = jnp.concatenate(
                [image[:, 2 * g * LANES:(2 * g + 1) * LANES], image[:, (2 * g + 1) * LANES:(2 * g + 2) * LANES]],
                axis=0,
            )
            both = jnp.dot(pair, bd_buf[a, g], preferred_element_type=F32)
            parts.append(both[0:LM, 0:LANES])
            parts.append(both[LM:2 * LM, LANES:])
        parts[0] = parts[0] + first_buf[a]
        return jnp.concatenate([part.astype(BF16) for part in parts], axis=1)

    def sweep(a, flat):
        img_buf[a] = jnp.dot(flat, st_buf[a], preferred_element_type=F32).astype(BF16)

    for step in range(SWEEPS - 1):
        for a in range(A_DEV):
            if step == 0:
                zone_blocks(a)
            sweep(a, zone(a))

    total = jnp.zeros((LANES, LANES), F32)
    pick = [ones_where((lane16 % LM) // 2 == h).astype(BF16) for h in range(8)]
    for a in range(A_DEV):
        image = img_buf[a]
        rows = jnp.concatenate([image * jnp.concatenate([pick[h]] * 8, axis=1) for h in range(8)], axis=0)
        total = total + jnp.dot(rows, q_buf[a], preferred_element_type=F32)
    g_send[...] = total.T

    def g_copy(place):
        return pltpu.make_async_remote_copy(
            src_ref=g_send.at[pl.ds(place * LM, LM)], dst_ref=g_land.at[2 * SPAN - place],
            send_sem=g_send_sem.at[place], recv_sem=g_recv_sem.at[2 * SPAN - place],
            device_id={"atom": atom_at(place - SPAN)}, device_id_type=MESH,
        )

    for place in others:
        g_copy(place).start()
    owned = g_send[SPAN * LM:(SPAN + 1) * LM, :]
    for place in others:
        g_copy(2 * SPAN - place).wait_recv()
        owned = owned + g_land[place]

    high = owned.astype(BF16)
    low = (owned - high.astype(F32)).astype(BF16)
    apart = ones_where(row // LM == lane // LM).astype(BF16)
    stacked = jnp.concatenate(
        [jnp.concatenate([high] * 8, axis=0) * apart, jnp.concatenate([low] * 8, axis=0) * apart], axis=0
    )
    received = jnp.dot(tbx_buf[...], stacked, preferred_element_type=F32)
    for by in (16, 32, 64):
        received = received + pltpu.roll(received, by, 1)
    received = received + t_tiled[...]
    received_b = received.astype(BF16) * apart
    rad_in.wait()
    radial = rad_ref[...]
    turned = jnp.dot(received_b, radial, preferred_element_type=F32)
    product = radial.astype(F32) * turned
    partial = product.reshape(A_DEV, LM, product.shape[1]).sum(axis=1) * w_ref[0]
    chunk = product.shape[1] // n_energy
    for e in range(n_energy):
        p_send[e] = partial[:, e * chunk:(e + 1) * chunk]

    def p_copy(by):
        return pltpu.make_async_remote_copy(
            src_ref=p_send.at[energy_at(by)], dst_ref=p_land.at[by - 1],
            send_sem=p_send_sem.at[by - 1], recv_sem=p_recv_sem.at[by - 1],
            device_id={"energy": energy_at(by)}, device_id_type=MESH,
        )

    for by in range(1, n_energy):
        p_copy(by).start()
    density = p_send[mine]
    for by in range(1, n_energy):
        p_copy(by).wait_recv()
        density = density + p_land[by - 1]
    out_ref[...] = density
    for place in others:
        g_copy(place).wait_send()
    for by in range(1, n_energy):
        p_copy(by).wait_send()


def shards(n_atom, n_energy, t_matrix, structure, radial, weights, neighbours, live):
    r = radial.shape[-1]
    vmem = pl.BlockSpec(memory_space=pltpu.VMEM)
    smem = pl.BlockSpec(memory_space=pltpu.SMEM)
    hbm = pl.BlockSpec(memory_space=pl.ANY)
    return pl.pallas_call(
        functools.partial(kernel, n_atom, n_energy),
        out_shape=jax.ShapeDtypeStruct((A_DEV, r // n_energy), F32),
        in_specs=[hbm, hbm, smem, hbm, hbm, hbm],
        out_specs=vmem,
        scratch_shapes=[
            pltpu.VMEM((A_DEV * LM, LM), F32),
            pltpu.VMEM((A_DEV * LM, r), BF16),
            pltpu.VMEM((A_DEV, NB), jnp.int32),
            pltpu.VMEM((A_DEV, NB), jnp.int32),
            pltpu.VMEM((A_DEV, NB), jnp.int32),
            pltpu.VMEM((PLACES * A_DEV + 8, LM, LANES), BF16),
            pltpu.VMEM((A_DEV, SIZE, SIZE), BF16),
            pltpu.VMEM((A_DEV, SIZE, SIZE), BF16),
            pltpu.VMEM((A_DEV, SIZE, LANES), BF16),
            pltpu.VMEM((A_DEV, 4, LANES, TILE), BF16),
            pltpu.VMEM((PLACES * A_DEV + 8, LM, LANES), BF16),
            pltpu.VMEM((LM, LANES), F32),
            pltpu.VMEM((PLACES, LM, LANES), F32),
            pltpu.VMEM((A_DEV, LM, LANES), F32),
            pltpu.VMEM((A_DEV, LM, SIZE), BF16),
            pltpu.VMEM((LANES, A_DEV * LANES), BF16),
            pltpu.VMEM((LANES, 2 * LANES), BF16),
            pltpu.VMEM((LANES, LANES), F32),
            pltpu.VMEM((LANES, LANES), F32),
            pltpu.VMEM((PLACES, LM, LANES), F32),
            pltpu.VMEM((n_energy, A_DEV, r // n_energy), F32),
            pltpu.VMEM((n_energy - 1, A_DEV, r // n_energy), F32),
            pltpu.SMEM((A_DEV, NB), jnp.int32),
            pltpu.SemaphoreType.DMA((5,)),
            pltpu.SemaphoreType.DMA((A_DEV,)),
            pltpu.SemaphoreType.DMA((PLACES,)),
            pltpu.SemaphoreType.DMA((PLACES,)),
            pltpu.SemaphoreType.DMA((PLACES,)),
            pltpu.SemaphoreType.DMA((PLACES,)),
            pltpu.SemaphoreType.DMA((n_energy - 1,)),
            pltpu.SemaphoreType.DMA((n_energy - 1,)),
        ],
        compiler_params=pltpu.CompilerParams(
            collective_id=0, has_side_effects=True, vmem_limit_bytes=60 * 1024 * 1024
        ),
    )(
        t_matrix.reshape(A_DEV * LM, LM),
        radial.reshape(A_DEV * LM, r),
        weights,
        neighbours,
        live,
        structure.reshape(A_DEV, SIZE, SIZE),
    )


def solution(mesh):
    in_specs = (
        P("energy", "atom", None, None),
        P("energy", "atom", None, None),
        P("energy", "atom", None, None),
        P("energy"),
        P("atom", None),
        P("atom", None),
    )
    body = functools.partial(shards, mesh.shape["atom"], mesh.shape["energy"])
    return jax.shard_map(body, mesh=mesh, in_specs=in_specs, out_specs=P("atom", "energy"), check_vma=False)
```

```python
import functools

import jax
import jax.numpy as jnp
from jax import lax
from jax.experimental import pallas as pl
from jax.experimental.pallas import tpu as pltpu
from jax.sharding import PartitionSpec as P

MESH = pl.DeviceIdType.MESH
F32 = jnp.float32
BF16 = jnp.bfloat16

SPAN = 3
PLACES = 2 * SPAN + 1
SWEEPS = 4
LM = 16
NB = 64
A_DEV = 8
LANES = 128
SIZE = NB * LM
TILE = 256
EARLY = 1


def iota(shape, dim):
    return lax.broadcasted_iota(jnp.int32, shape, dim)


def ones_where(cond):
    return jnp.where(cond, 1.0, 0.0).astype(F32)


def kernel(
    n_atom, n_energy,
    t_hbm, rad_hbm, w_hbm, nbr_hbm, live_hbm, s_hbm, out_ref,
    t_ref, rad_ref, w_ref, nbr_ref, live_ref, slot_vec, pattern, s_buf, st_buf, q_buf, bd_buf, table, t_self, t_land, first_buf, img_buf, spread_buf, tbx_buf, t_tiled,
    g_send, g_land, p_send, p_land, slot_of,
    in_sem, s_sem, t_send_sem, t_recv_sem, g_send_sem, g_recv_sem, p_send_sem, p_recv_sem,
):
    me = lax.axis_index("atom")
    mine = lax.axis_index("energy")

    def atom_at(by):
        return lax.rem(me + by + n_atom, n_atom)

    def energy_at(by):
        return lax.rem(mine + by, n_energy)

    others = [place for place in range(PLACES) if place != SPAN]

    t_in = pltpu.make_async_copy(t_hbm, t_ref, in_sem.at[0])
    nbr_in = pltpu.make_async_copy(nbr_hbm, nbr_ref, in_sem.at[1])
    live_in = pltpu.make_async_copy(live_hbm, live_ref, in_sem.at[2])
    rad_in = pltpu.make_async_copy(rad_hbm, rad_ref, in_sem.at[3])
    w_in = pltpu.make_async_copy(w_hbm, w_ref, in_sem.at[5])
    t_in.start()
    nbr_in.start()
    live_in.start()

    barrier = pltpu.get_barrier_semaphore()
    for place in others:
        pl.semaphore_signal(barrier, inc=1, device_id={"atom": atom_at(place - SPAN)}, device_id_type=MESH)
    for by in range(1, n_energy):
        pl.semaphore_signal(barrier, inc=1, device_id={"energy": energy_at(by)}, device_id_type=MESH)

    def s_copy(a):
        return pltpu.make_async_copy(s_hbm.at[a], s_buf.at[a], s_sem.at[a])

    for a in range(A_DEV):
        s_copy(a).start()
    rad_in.start()
    w_in.start()

    t_in.wait()
    t_rows = t_ref[...]
    t_wide = jnp.concatenate([t_rows, jnp.zeros((A_DEV * LM, LANES - LM), F32)], axis=1)
    t_turned = t_wide.T[0:LM, :]
    t_self[...] = t_turned
    lane16 = iota((LM, LANES), 1)
    for a in range(A_DEV):
        moved = t_turned if a == 0 else pltpu.roll(t_turned, LANES - a * LM, 1)
        first_buf[a] = jnp.where(lane16 < LM, moved, 0.0)

    nbr_in.wait()
    live_in.wait()
    nbr = nbr_ref[...]
    place = lax.rem(nbr // A_DEV - me + SPAN + n_atom, n_atom)
    slot_vec[...] = jnp.where(live_ref[...] > 0, place * A_DEV + lax.rem(nbr, A_DEV), PLACES * A_DEV)
    slot_out = pltpu.make_async_copy(slot_vec, slot_of, in_sem.at[4])
    slot_out.start()

    def turn(a, carry):
        s_copy(a).wait()
        for bi in range(SIZE // TILE):
            for bj in range(SIZE // TILE):
                st_buf[a, bj * TILE:(bj + 1) * TILE, bi * TILE:(bi + 1) * TILE] = s_buf[
                    a, bi * TILE:(bi + 1) * TILE, bj * TILE:(bj + 1) * TILE
                ].T
        img_buf[a] = jnp.dot(
            first_buf[a].astype(BF16), st_buf[a, 0:LANES, :], preferred_element_type=F32
        ).astype(BF16)
        return carry

    lane = iota((LANES, LANES), 1)
    row = iota((LANES, LANES), 0)
    t_b = t_rows.astype(BF16)
    expand = ones_where(iota((LM, LANES), 1) // A_DEV == iota((LM, LANES), 0)).astype(BF16)
    tbx = jnp.dot(t_b, expand, preferred_element_type=F32)
    tbx = jnp.where(lane % A_DEV == row // LM, tbx, 0.0).astype(BF16)
    tbx_buf[:, 0:LANES] = tbx
    tbx_buf[:, LANES:] = tbx
    tiled = t_wide
    for by in (16, 32, 64):
        tiled = tiled + pltpu.roll(tiled, by, 1)
    t_tiled[...] = tiled
    for a in range(A_DEV):
        spread_buf[:, a * LANES:(a + 1) * LANES] = ones_where(
            (row // LM == a) & (row % LM == lane % LM)
        ).astype(BF16)

    lax.fori_loop(0, EARLY, turn, 0)
    pl.semaphore_wait(barrier, len(others) + n_energy - 1)

    def t_copy(place):
        return pltpu.make_async_remote_copy(
            src_ref=t_self, dst_ref=t_land.at[2 * SPAN - place],
            send_sem=t_send_sem.at[place], recv_sem=t_recv_sem.at[2 * SPAN - place],
            device_id={"atom": atom_at(place - SPAN)}, device_id_type=MESH,
        )

    for place in others:
        t_copy(place).start()

    where_to = lane16 - A_DEV * (iota((LM, LANES), 0) % 2)
    for place in range(PLACES):
        for a in range(A_DEV):
            pattern[place * A_DEV + a] = ones_where(where_to == place * LM + a).astype(BF16)
    pattern[PLACES * A_DEV] = jnp.zeros((LM, LANES), BF16)
    slot_out.wait()

    def hot(a, carry):
        for s in range(NB):
            q_buf[a, s * LM:(s + 1) * LM, :] = pattern[slot_of[a, s]]
        return carry

    lax.fori_loop(0, A_DEV, hot, 0)

    lax.fori_loop(EARLY, A_DEV, turn, 0)


    t_land[SPAN] = t_self[...]
    for place in others:
        t_copy(place).wait_send()
        t_copy(2 * SPAN - place).wait_recv()
    landed = t_land[...].reshape(PLACES * LM, LANES).astype(BF16)
    wide = jnp.dot(landed, spread_buf[...], preferred_element_type=F32).astype(BF16)
    for place in range(PLACES):
        for a in range(A_DEV):
            table[place * A_DEV + a] = wide[place * LM:(place + 1) * LM, a * LANES:(a + 1) * LANES]
    table[PLACES * A_DEV] = jnp.zeros((LM, LANES), BF16)

    keep = [ones_where(lane16 // LM == r).astype(BF16) for r in range(8)]

    def zone_blocks(a):
        for g in range(4):
            for h in range(2):
                for r in range(8):
                    s = g * 16 + h * 8 + r
                    bd_buf[a, g, r * LM:(r + 1) * LM, h * LANES:(h + 1) * LANES] = (
                        table[slot_of[a, s]] * keep[r]
                    )

    def zone(a):
        image = img_buf[a]
        parts = []
        for g in range(4):
            pair = jnp.concatenate(
                [image[:, 2 * g * LANES:(2 * g + 1) * LANES], image[:, (2 * g + 1) * LANES:(2 * g + 2) * LANES]],
                axis=0,
            )
            both = jnp.dot(pair, bd_buf[a, g], preferred_element_type=F32)
            parts.append(both[0:LM, 0:LANES])
            parts.append(both[LM:2 * LM, LANES:])
        parts[0] = parts[0] + first_buf[a]
        return jnp.concatenate([part.astype(BF16) for part in parts], axis=1)

    def sweep(a, flat):
        img_buf[a] = jnp.dot(flat, st_buf[a], preferred_element_type=F32).astype(BF16)

    pick = [ones_where((lane16 % LM) // 2 == h).astype(BF16) for h in range(8)]

    def zone_sum(a):
        image = img_buf[a]
        rows = jnp.concatenate([image * jnp.concatenate([pick[h]] * 8, axis=1) for h in range(8)], axis=0)
        return jnp.dot(rows, q_buf[a], preferred_element_type=F32)

    order = [(step, a) for step in range(SWEEPS - 1) for a in range(A_DEV)]
    zone_blocks(0)
    flat = zone(0)
    total = jnp.zeros((LANES, LANES), F32)
    for n, (step, a) in enumerate(order):
        ahead = None
        if n + 1 < len(order):
            if order[n + 1][0] == 0:
                zone_blocks(order[n + 1][1])
            ahead = zone(order[n + 1][1])
        if step == SWEEPS - 2 and a > 0:
            total = total + zone_sum(a - 1)
        sweep(a, flat)
        flat = ahead
    total = total + zone_sum(A_DEV - 1)
    g_send[...] = total.T

    def g_copy(place):
        return pltpu.make_async_remote_copy(
            src_ref=g_send.at[pl.ds(place * LM, LM)], dst_ref=g_land.at[2 * SPAN - place],
            send_sem=g_send_sem.at[place], recv_sem=g_recv_sem.at[2 * SPAN - place],
            device_id={"atom": atom_at(place - SPAN)}, device_id_type=MESH,
        )

    for place in others:
        g_copy(place).start()
    owned = g_send[SPAN * LM:(SPAN + 1) * LM, :]
    for place in others:
        g_copy(2 * SPAN - place).wait_recv()
        owned = owned + g_land[place]

    high = owned.astype(BF16)
    low = (owned - high.astype(F32)).astype(BF16)
    apart = ones_where(row // LM == lane // LM).astype(BF16)
    stacked = jnp.concatenate(
        [jnp.concatenate([high] * 8, axis=0) * apart, jnp.concatenate([low] * 8, axis=0) * apart], axis=0
    )
    received = jnp.dot(tbx_buf[...], stacked, preferred_element_type=F32)
    for by in (16, 32, 64):
        received = received + pltpu.roll(received, by, 1)
    received = received + t_tiled[...]
    received_b = received.astype(BF16) * apart
    rad_in.wait()
    w_in.wait()
    radial = rad_ref[...]
    turned = jnp.dot(received_b, radial, preferred_element_type=F32)
    product = radial.astype(F32) * turned
    partial = product.reshape(A_DEV, LM, product.shape[1]).sum(axis=1) * w_ref[0]
    chunk = product.shape[1] // n_energy
    for e in range(n_energy):
        p_send[e] = partial[:, e * chunk:(e + 1) * chunk]

    def p_copy(by):
        return pltpu.make_async_remote_copy(
            src_ref=p_send.at[energy_at(by)], dst_ref=p_land.at[by - 1],
            send_sem=p_send_sem.at[by - 1], recv_sem=p_recv_sem.at[by - 1],
            device_id={"energy": energy_at(by)}, device_id_type=MESH,
        )

    for by in range(1, n_energy):
        p_copy(by).start()
    density = p_send[mine]
    for by in range(1, n_energy):
        p_copy(by).wait_recv()
        density = density + p_land[by - 1]
    out_ref[...] = density
    for place in others:
        g_copy(place).wait_send()
    for by in range(1, n_energy):
        p_copy(by).wait_send()


def shards(n_atom, n_energy, t_matrix, structure, radial, weights, neighbours, live):
    r = radial.shape[-1]
    vmem = pl.BlockSpec(memory_space=pltpu.VMEM)
    hbm = pl.BlockSpec(memory_space=pl.ANY)
    return pl.pallas_call(
        functools.partial(kernel, n_atom, n_energy),
        out_shape=pltpu.VMEM((A_DEV, r // n_energy), F32),
        in_specs=[hbm] * 6,
        out_specs=vmem,
        scratch_shapes=[
            pltpu.VMEM((A_DEV * LM, LM), F32),
            pltpu.VMEM((A_DEV * LM, r), BF16),
            pltpu.SMEM((1,), F32),
            pltpu.VMEM((A_DEV, NB), jnp.int32),
            pltpu.VMEM((A_DEV, NB), jnp.int32),
            pltpu.VMEM((A_DEV, NB), jnp.int32),
            pltpu.VMEM((PLACES * A_DEV + 8, LM, LANES), BF16),
            pltpu.VMEM((A_DEV, SIZE, SIZE), BF16),
            pltpu.VMEM((A_DEV, SIZE, SIZE), BF16),
            pltpu.VMEM((A_DEV, SIZE, LANES), BF16),
            pltpu.VMEM((A_DEV, 4, LANES, TILE), BF16),
            pltpu.VMEM((PLACES * A_DEV + 8, LM, LANES), BF16),
            pltpu.VMEM((LM, LANES), F32),
            pltpu.VMEM((PLACES, LM, LANES), F32),
            pltpu.VMEM((A_DEV, LM, LANES), F32),
            pltpu.VMEM((A_DEV, LM, SIZE), BF16),
            pltpu.VMEM((LANES, A_DEV * LANES), BF16),
            pltpu.VMEM((LANES, 2 * LANES), BF16),
            pltpu.VMEM((LANES, LANES), F32),
            pltpu.VMEM((LANES, LANES), F32),
            pltpu.VMEM((PLACES, LM, LANES), F32),
            pltpu.VMEM((n_energy, A_DEV, r // n_energy), F32),
            pltpu.VMEM((n_energy - 1, A_DEV, r // n_energy), F32),
            pltpu.SMEM((A_DEV, NB), jnp.int32),
            pltpu.SemaphoreType.DMA((6,)),
            pltpu.SemaphoreType.DMA((A_DEV,)),
            pltpu.SemaphoreType.DMA((PLACES,)),
            pltpu.SemaphoreType.DMA((PLACES,)),
            pltpu.SemaphoreType.DMA((PLACES,)),
            pltpu.SemaphoreType.DMA((PLACES,)),
            pltpu.SemaphoreType.DMA((n_energy - 1,)),
            pltpu.SemaphoreType.DMA((n_energy - 1,)),
        ],
        compiler_params=pltpu.CompilerParams(
            collective_id=0, has_side_effects=True, vmem_limit_bytes=60 * 1024 * 1024
        ),
    )(
        t_matrix.reshape(A_DEV * LM, LM),
        radial.reshape(A_DEV * LM, r),
        weights,
        neighbours,
        live,
        structure.reshape(A_DEV, SIZE, SIZE),
    )


def solution(mesh):
    in_specs = (
        P("energy", "atom", None, None),
        P("energy", "atom", None, None),
        P("energy", "atom", None, None),
        P("energy"),
        P("atom", None),
        P("atom", None),
    )
    body = functools.partial(shards, mesh.shape["atom"], mesh.shape["energy"])
    return jax.shard_map(body, mesh=mesh, in_specs=in_specs, out_specs=P("atom", "energy"), check_vma=False)
```

```python
import functools

import jax
import jax.numpy as jnp
from jax import lax
from jax.experimental import pallas as pl
from jax.experimental.pallas import tpu as pltpu
from jax.sharding import PartitionSpec as P

MESH = pl.DeviceIdType.MESH
F32 = jnp.float32
BF16 = jnp.bfloat16

SPAN = 3
PLACES = 2 * SPAN + 1
SWEEPS = 4
LM = 16
NB = 64
A_DEV = 8
LANES = 128
SIZE = NB * LM
TILE = 256
EARLY = 0
MIDDLE = 3
ROW = 8


def iota(shape, dim):
    return lax.broadcasted_iota(jnp.int32, shape, dim)


def ones_where(cond):
    return jnp.where(cond, 1.0, 0.0).astype(F32)


def kernel(
    n_atom, n_energy,
    t_hbm, rad_hbm, w_hbm, nbr_hbm, live_hbm, s_hbm, out_ref,
    t_ref, rad_ref, w_ref, nbr_ref, live_ref, slot_vec, pattern, s_buf, st_buf, q_buf, bd_buf, table, t_self, t_land, first_buf, img_buf, spread_buf, tbx_buf, t_tiled,
    g_send, g_land, p_send, p_land, slot_of,
    same, fed, feed_sem, ready, in_sem, s_sem, t_send_sem, t_recv_sem, g_send_sem, g_recv_sem, p_send_sem, p_recv_sem,
):
    me = lax.axis_index("atom")
    mine = lax.axis_index("energy")

    def atom_at(by):
        return lax.rem(me + by + n_atom, n_atom)

    def energy_at(by):
        return lax.rem(mine + by, n_energy)

    others = [place for place in range(PLACES) if place != SPAN]

    t_in = pltpu.make_async_copy(t_hbm, t_ref, in_sem.at[0])
    nbr_in = pltpu.make_async_copy(nbr_hbm, nbr_ref, in_sem.at[1])
    live_in = pltpu.make_async_copy(live_hbm, live_ref, in_sem.at[2])
    rad_in = pltpu.make_async_copy(rad_hbm, rad_ref, in_sem.at[3])
    w_in = pltpu.make_async_copy(w_hbm, w_ref, in_sem.at[5])
    t_in.start()
    nbr_in.start()
    live_in.start()

    barrier = pltpu.get_barrier_semaphore()
    spot = lax.rem(me, ROW)

    def greet(by):
        pl.semaphore_signal(barrier, inc=1, device_id={"atom": atom_at(by)}, device_id_type=MESH)

    for d in range(1, SPAN + 1):
        greet(-d)
        pl.when(spot + d < ROW)(functools.partial(greet, d))
        pl.when(spot < d)(functools.partial(greet, ROW - d))
    greet(ROW)
    for by in range(1, n_energy):
        pl.semaphore_signal(barrier, inc=1, device_id={"energy": energy_at(by)}, device_id_type=MESH)

    def s_copy(a):
        return pltpu.make_async_copy(s_hbm.at[a], s_buf.at[a], s_sem.at[a])

    for a in range(A_DEV):
        s_copy(a).start()
    rad_in.start()
    w_in.start()

    t_in.wait()
    t_rows = t_ref[...]
    t_wide = jnp.concatenate([t_rows, jnp.zeros((A_DEV * LM, LANES - LM), F32)], axis=1)
    t_turned = t_wide.T[0:LM, :]
    t_self[...] = t_turned
    lane16 = iota((LM, LANES), 1)
    for a in range(A_DEV):
        moved = t_turned if a == 0 else pltpu.roll(t_turned, LANES - a * LM, 1)
        first_buf[a] = jnp.where(lane16 < LM, moved, 0.0)

    nbr_in.wait()
    live_in.wait()
    nbr = nbr_ref[...]
    place = lax.rem(nbr // A_DEV - me + SPAN + n_atom, n_atom)
    slot_vec[...] = jnp.where(live_ref[...] > 0, place * A_DEV + lax.rem(nbr, A_DEV), PLACES * A_DEV)
    slot_out = pltpu.make_async_copy(slot_vec, slot_of, in_sem.at[4])
    slot_out.start()

    same[...] = ones_where(iota((TILE, TILE), 0) == iota((TILE, TILE), 1)).astype(BF16)

    def turn(a, carry):
        s_copy(a).wait()
        for bi in range(SIZE // TILE):
            for bj in range(SIZE // TILE):
                tile = s_buf[a, bi * TILE:(bi + 1) * TILE, bj * TILE:(bj + 1) * TILE]
                if (bi * 4 + bj) % 3 == 1:
                    tile = lax.dot_general(
                        same[...], tile, (((1,), (1,)), ((), ())), preferred_element_type=F32
                    ).astype(BF16)
                else:
                    tile = tile.T
                st_buf[a, bj * TILE:(bj + 1) * TILE, bi * TILE:(bi + 1) * TILE] = tile
        img_buf[a] = jnp.dot(
            first_buf[a].astype(BF16), st_buf[a, 0:LANES, :], preferred_element_type=F32
        ).astype(BF16)
        return carry

    lane = iota((LANES, LANES), 1)
    row = iota((LANES, LANES), 0)
    t_b = t_rows.astype(BF16)
    expand = ones_where(iota((LM, LANES), 1) // A_DEV == iota((LM, LANES), 0)).astype(BF16)
    tbx = jnp.dot(t_b, expand, preferred_element_type=F32)
    tbx = jnp.where(lane % A_DEV == row // LM, tbx, 0.0).astype(BF16)
    tbx_buf[:, 0:LANES] = tbx
    tbx_buf[:, LANES:] = tbx
    tiled = t_wide
    for by in (16, 32, 64):
        tiled = tiled + pltpu.roll(tiled, by, 1)
    t_tiled[...] = tiled
    for a in range(A_DEV):
        spread_buf[:, a * LANES:(a + 1) * LANES] = ones_where(
            (row // LM == a) & (row % LM == lane % LM)
        ).astype(BF16)

    lax.fori_loop(0, EARLY, turn, 0)
    greeted = SPAN + jnp.minimum(spot, SPAN) + jnp.maximum(spot + SPAN + 1 - ROW, 0) + 1 + n_energy - 1
    pl.semaphore_wait(barrier, greeted)

    def t_copy(src, by, place):
        return pltpu.make_async_remote_copy(
            src_ref=src, dst_ref=t_land.at[place],
            send_sem=t_send_sem.at[place], recv_sem=t_recv_sem.at[place],
            device_id={"atom": atom_at(by)}, device_id_type=MESH,
        )

    def feed():
        return pltpu.make_async_remote_copy(
            src_ref=t_self, dst_ref=fed, send_sem=feed_sem.at[0], recv_sem=feed_sem.at[1],
            device_id={"atom": atom_at(-ROW)}, device_id_type=MESH,
        )

    def t_down(d):
        t_copy(t_self, -d, SPAN + d).start()

    def ask(d):
        pl.semaphore_signal(ready.at[d - 1], inc=1, device_id={"atom": atom_at(d - ROW)}, device_id_type=MESH)

    feed().start()
    for d in range(1, SPAN + 1):
        pl.when(spot + d >= ROW)(functools.partial(ask, d))
    for d in range(1, SPAN + 1):
        t_copy(t_self, d, SPAN - d).start()
        pl.when(spot >= d)(functools.partial(t_down, d))

    where_to = lane16 - A_DEV * (iota((LM, LANES), 0) % 2)
    for place in range(PLACES):
        for a in range(A_DEV):
            pattern[place * A_DEV + a] = ones_where(where_to == place * LM + a).astype(BF16)
    pattern[PLACES * A_DEV] = jnp.zeros((LM, LANES), BF16)
    slot_out.wait()

    def hot(a, carry):
        for s in range(NB):
            q_buf[a, s * LM:(s + 1) * LM, :] = pattern[slot_of[a, s]]
        return carry

    lax.fori_loop(0, A_DEV, hot, 0)

    lax.fori_loop(EARLY, MIDDLE, turn, 0)

    def forward(d):
        pl.semaphore_wait(ready.at[d - 1], 1)
        t_copy(fed, ROW - d, SPAN + d).start()

    pl.when(spot < SPAN)(lambda: feed().wait_recv())
    for d in range(SPAN, 0, -1):
        pl.when(spot < d)(functools.partial(forward, d))
    lax.fori_loop(MIDDLE, A_DEV, turn, 0)


    t_land[SPAN] = t_self[...]
    for place in others:
        t_copy(t_self, place - SPAN, place).wait_recv()
    landed = t_land[...].reshape(PLACES * LM, LANES).astype(BF16)
    wide = jnp.dot(landed, spread_buf[...], preferred_element_type=F32).astype(BF16)
    for place in range(PLACES):
        for a in range(A_DEV):
            table[place * A_DEV + a] = wide[place * LM:(place + 1) * LM, a * LANES:(a + 1) * LANES]
    table[PLACES * A_DEV] = jnp.zeros((LM, LANES), BF16)

    keep = [ones_where(lane16 // LM == r).astype(BF16) for r in range(8)]

    def zone_blocks(a):
        for g in range(4):
            for h in range(2):
                for r in range(8):
                    s = g * 16 + h * 8 + r
                    bd_buf[a, g, r * LM:(r + 1) * LM, h * LANES:(h + 1) * LANES] = (
                        table[slot_of[a, s]] * keep[r]
                    )

    def zone(a):
        image = img_buf[a]
        parts = []
        for g in range(4):
            pair = jnp.concatenate(
                [image[:, 2 * g * LANES:(2 * g + 1) * LANES], image[:, (2 * g + 1) * LANES:(2 * g + 2) * LANES]],
                axis=0,
            )
            both = jnp.dot(pair, bd_buf[a, g], preferred_element_type=F32)
            parts.append(both[0:LM, 0:LANES])
            parts.append(both[LM:2 * LM, LANES:])
        parts[0] = parts[0] + first_buf[a]
        return jnp.concatenate([part.astype(BF16) for part in parts], axis=1)

    def sweep(a, flat):
        img_buf[a] = jnp.dot(flat, st_buf[a], preferred_element_type=F32).astype(BF16)

    pick = [ones_where((lane16 % LM) // 2 == h).astype(BF16) for h in range(8)]

    def zone_sum(a):
        image = img_buf[a]
        rows = jnp.concatenate([image * jnp.concatenate([pick[h]] * 8, axis=1) for h in range(8)], axis=0)
        return jnp.dot(rows, q_buf[a], preferred_element_type=F32)

    order = [(step, a) for step in range(SWEEPS - 1) for a in range(A_DEV)]
    zone_blocks(0)
    flat = zone(0)
    total = jnp.zeros((LANES, LANES), F32)
    for n, (step, a) in enumerate(order):
        ahead = None
        if n + 1 < len(order):
            if order[n + 1][0] == 0:
                zone_blocks(order[n + 1][1])
            ahead = zone(order[n + 1][1])
        if step == SWEEPS - 2 and a > 0:
            total = total + zone_sum(a - 1)
        sweep(a, flat)
        flat = ahead
    total = total + zone_sum(A_DEV - 1)
    g_send[...] = total.T

    def g_copy(place):
        return pltpu.make_async_remote_copy(
            src_ref=g_send.at[pl.ds(place * LM, LM)], dst_ref=g_land.at[2 * SPAN - place],
            send_sem=g_send_sem.at[place], recv_sem=g_recv_sem.at[2 * SPAN - place],
            device_id={"atom": atom_at(place - SPAN)}, device_id_type=MESH,
        )

    for place in others:
        g_copy(place).start()
    owned = g_send[SPAN * LM:(SPAN + 1) * LM, :]
    for place in others:
        g_copy(2 * SPAN - place).wait_recv()
        owned = owned + g_land[place]

    apart = ones_where(row // LM == lane // LM).astype(BF16)
    moved = [owned if d == 0 else pltpu.roll(owned, d * LM, 1) for d in range(8)]
    blocks = []
    for h in range(8):
        block = moved[(8 - h) % 8]
        for x in range(1, 8):
            block = jnp.where(lane16 // LM == x, moved[(x - h) % 8], block)
        blocks.append(block)
    owned_rows = jnp.concatenate(blocks, axis=0)
    high = owned_rows.astype(BF16)
    low = (owned_rows - high.astype(F32)).astype(BF16)
    received = jnp.dot(tbx_buf[...], jnp.concatenate([high, low], axis=0), preferred_element_type=F32)
    received_b = (received + t_tiled[...]).astype(BF16) * apart
    rad_in.wait()
    w_in.wait()
    radial = rad_ref[...]
    turned = jnp.dot(received_b, radial, preferred_element_type=F32)
    product = radial.astype(F32) * turned
    partial = product.reshape(A_DEV, LM, product.shape[1]).sum(axis=1) * w_ref[0]
    chunk = product.shape[1] // n_energy
    for e in range(n_energy):
        p_send[e] = partial[:, e * chunk:(e + 1) * chunk]

    def p_copy(by):
        return pltpu.make_async_remote_copy(
            src_ref=p_send.at[energy_at(by)], dst_ref=p_land.at[by - 1],
            send_sem=p_send_sem.at[by - 1], recv_sem=p_recv_sem.at[by - 1],
            device_id={"energy": energy_at(by)}, device_id_type=MESH,
        )

    for by in range(1, n_energy):
        p_copy(by).start()
    density = p_send[mine]
    for by in range(1, n_energy):
        p_copy(by).wait_recv()
        density = density + p_land[by - 1]
    out_ref[...] = density
    pl.when(spot >= SPAN)(lambda: feed().wait_recv())
    feed().wait_send()
    for place in others:
        t_copy(t_self, place - SPAN, place).wait_send()
        g_copy(place).wait_send()
    for by in range(1, n_energy):
        p_copy(by).wait_send()


def shards(n_atom, n_energy, t_matrix, structure, radial, weights, neighbours, live):
    r = radial.shape[-1]
    vmem = pl.BlockSpec(memory_space=pltpu.VMEM)
    hbm = pl.BlockSpec(memory_space=pl.ANY)
    return pl.pallas_call(
        functools.partial(kernel, n_atom, n_energy),
        out_shape=pltpu.VMEM((A_DEV, r // n_energy), F32),
        in_specs=[hbm] * 6,
        out_specs=vmem,
        scratch_shapes=[
            pltpu.VMEM((A_DEV * LM, LM), F32),
            pltpu.VMEM((A_DEV * LM, r), BF16),
            pltpu.SMEM((1,), F32),
            pltpu.VMEM((A_DEV, NB), jnp.int32),
            pltpu.VMEM((A_DEV, NB), jnp.int32),
            pltpu.VMEM((A_DEV, NB), jnp.int32),
            pltpu.VMEM((PLACES * A_DEV + 8, LM, LANES), BF16),
            pltpu.VMEM((A_DEV, SIZE, SIZE), BF16),
            pltpu.VMEM((A_DEV, SIZE, SIZE), BF16),
            pltpu.VMEM((A_DEV, SIZE, LANES), BF16),
            pltpu.VMEM((A_DEV, 4, LANES, TILE), BF16),
            pltpu.VMEM((PLACES * A_DEV + 8, LM, LANES), BF16),
            pltpu.VMEM((LM, LANES), F32),
            pltpu.VMEM((PLACES, LM, LANES), F32),
            pltpu.VMEM((A_DEV, LM, LANES), F32),
            pltpu.VMEM((A_DEV, LM, SIZE), BF16),
            pltpu.VMEM((LANES, A_DEV * LANES), BF16),
            pltpu.VMEM((LANES, 2 * LANES), BF16),
            pltpu.VMEM((LANES, LANES), F32),
            pltpu.VMEM((LANES, LANES), F32),
            pltpu.VMEM((PLACES, LM, LANES), F32),
            pltpu.VMEM((n_energy, A_DEV, r // n_energy), F32),
            pltpu.VMEM((n_energy - 1, A_DEV, r // n_energy), F32),
            pltpu.SMEM((A_DEV, NB), jnp.int32),
            pltpu.VMEM((TILE, TILE), BF16),
            pltpu.VMEM((LM, LANES), F32),
            pltpu.SemaphoreType.DMA((2,)),
            pltpu.SemaphoreType.REGULAR((SPAN,)),
            pltpu.SemaphoreType.DMA((6,)),
            pltpu.SemaphoreType.DMA((A_DEV,)),
            pltpu.SemaphoreType.DMA((PLACES,)),
            pltpu.SemaphoreType.DMA((PLACES,)),
            pltpu.SemaphoreType.DMA((PLACES,)),
            pltpu.SemaphoreType.DMA((PLACES,)),
            pltpu.SemaphoreType.DMA((n_energy - 1,)),
            pltpu.SemaphoreType.DMA((n_energy - 1,)),
        ],
        compiler_params=pltpu.CompilerParams(
            collective_id=0, has_side_effects=True, vmem_limit_bytes=60 * 1024 * 1024
        ),
    )(
        t_matrix.reshape(A_DEV * LM, LM),
        radial.reshape(A_DEV * LM, r),
        weights,
        neighbours,
        live,
        structure.reshape(A_DEV, SIZE, SIZE),
    )


def solution(mesh):
    in_specs = (
        P("energy", "atom", None, None),
        P("energy", "atom", None, None),
        P("energy", "atom", None, None),
        P("energy"),
        P("atom", None),
        P("atom", None),
    )
    body = functools.partial(shards, mesh.shape["atom"], mesh.shape["energy"])
    return jax.shard_map(body, mesh=mesh, in_specs=in_specs, out_specs=P("atom", "energy"), check_vma=False)
```

```python
import functools

import jax
import jax.numpy as jnp
from jax import lax
from jax.experimental import pallas as pl
from jax.experimental.pallas import tpu as pltpu
from jax.sharding import PartitionSpec as P

MESH = pl.DeviceIdType.MESH
F32 = jnp.float32
BF16 = jnp.bfloat16

SPAN = 3
PLACES = 2 * SPAN + 1
SWEEPS = 4
LM = 16
NB = 64
A_DEV = 8
LANES = 128
SIZE = NB * LM
TILE = 256
EARLY = 0
MIDDLE = 3
ROW = 8


def iota(shape, dim):
    return lax.broadcasted_iota(jnp.int32, shape, dim)


def ones_where(cond):
    return jnp.where(cond, 1.0, 0.0).astype(F32)


def kernel(
    n_atom, n_energy,
    t_hbm, rad_hbm, w_hbm, nbr_hbm, live_hbm, s_hbm, out_ref,
    t_ref, rad_ref, w_ref, nbr_ref, live_ref, slot_vec, pattern, s_buf, st_buf, q_buf, bd_buf, table, t_self, t_land, first_buf, img_buf, spread_buf, tbx_buf, t_tiled,
    g_send, g_land, p_send, p_land, slot_of,
    same, fed, feed_sem, ready, in_sem, s_sem, t_send_sem, t_recv_sem, g_send_sem, g_recv_sem, p_send_sem, p_recv_sem,
):
    me = lax.axis_index("atom")
    mine = lax.axis_index("energy")

    def atom_at(by):
        return lax.rem(me + by + n_atom, n_atom)

    def energy_at(by):
        return lax.rem(mine + by, n_energy)

    others = [place for place in range(PLACES) if place != SPAN]

    t_in = pltpu.make_async_copy(t_hbm, t_ref, in_sem.at[0])
    nbr_in = pltpu.make_async_copy(nbr_hbm, nbr_ref, in_sem.at[1])
    live_in = pltpu.make_async_copy(live_hbm, live_ref, in_sem.at[2])
    rad_in = pltpu.make_async_copy(rad_hbm, rad_ref, in_sem.at[3])
    w_in = pltpu.make_async_copy(w_hbm, w_ref, in_sem.at[5])
    t_in.start()
    nbr_in.start()
    live_in.start()

    barrier = pltpu.get_barrier_semaphore()
    spot = lax.rem(me, ROW)

    def greet(by):
        pl.semaphore_signal(barrier, inc=1, device_id={"atom": atom_at(by)}, device_id_type=MESH)

    for d in range(1, SPAN + 1):
        greet(-d)
        pl.when(spot + d < ROW)(functools.partial(greet, d))
        pl.when(spot < d)(functools.partial(greet, ROW - d))
    greet(ROW)
    for by in range(1, n_energy):
        pl.semaphore_signal(barrier, inc=1, device_id={"energy": energy_at(by)}, device_id_type=MESH)

    def s_copy(a):
        return pltpu.make_async_copy(s_hbm.at[a], s_buf.at[a], s_sem.at[a])

    for a in range(A_DEV):
        s_copy(a).start()
    rad_in.start()
    w_in.start()

    t_in.wait()
    t_rows = t_ref[...]
    t_wide = jnp.concatenate([t_rows, jnp.zeros((A_DEV * LM, LANES - LM), F32)], axis=1)
    t_turned = t_wide.T[0:LM, :]
    t_self[...] = t_turned
    lane16 = iota((LM, LANES), 1)
    for a in range(A_DEV):
        moved = t_turned if a == 0 else pltpu.roll(t_turned, LANES - a * LM, 1)
        first_buf[a] = jnp.where(lane16 < LM, moved, 0.0)

    nbr_in.wait()
    live_in.wait()
    nbr = nbr_ref[...]
    place = lax.rem(nbr // A_DEV - me + SPAN + n_atom, n_atom)
    slot_vec[...] = jnp.where(live_ref[...] > 0, place * A_DEV + lax.rem(nbr, A_DEV), PLACES * A_DEV)
    slot_out = pltpu.make_async_copy(slot_vec, slot_of, in_sem.at[4])
    slot_out.start()

    same[...] = ones_where(iota((TILE, TILE), 0) == iota((TILE, TILE), 1)).astype(BF16)

    def turn(a, carry):
        s_copy(a).wait()
        for bi in range(SIZE // TILE):
            for bj in range(SIZE // TILE):
                tile = s_buf[a, bi * TILE:(bi + 1) * TILE, bj * TILE:(bj + 1) * TILE]
                if (bi * 4 + bj) % 3 == 1:
                    tile = lax.dot_general(
                        same[...], tile, (((1,), (1,)), ((), ())), preferred_element_type=F32
                    ).astype(BF16)
                else:
                    tile = tile.T
                st_buf[a, bj * TILE:(bj + 1) * TILE, bi * TILE:(bi + 1) * TILE] = tile
        img_buf[a] = jnp.dot(
            first_buf[a].astype(BF16), st_buf[a, 0:LANES, :], preferred_element_type=F32
        ).astype(BF16)
        return carry

    lane = iota((LANES, LANES), 1)
    row = iota((LANES, LANES), 0)
    t_b = t_rows.astype(BF16)
    expand = ones_where(iota((LM, LANES), 1) // A_DEV == iota((LM, LANES), 0)).astype(BF16)
    tbx = jnp.dot(t_b, expand, preferred_element_type=F32)
    tbx = jnp.where(lane % A_DEV == row // LM, tbx, 0.0).astype(BF16)
    tbx_buf[:, 0:LANES] = tbx
    tbx_buf[:, LANES:] = tbx
    tiled = t_wide
    for by in (16, 32, 64):
        tiled = tiled + pltpu.roll(tiled, by, 1)
    t_tiled[...] = tiled
    for a in range(A_DEV):
        spread_buf[:, a * LANES:(a + 1) * LANES] = ones_where(
            (row // LM == a) & (row % LM == lane % LM)
        ).astype(BF16)

    lax.fori_loop(0, EARLY, turn, 0)
    greeted = SPAN + jnp.minimum(spot, SPAN) + jnp.maximum(spot + SPAN + 1 - ROW, 0) + 1 + n_energy - 1
    pl.semaphore_wait(barrier, greeted)

    def t_copy(src, by, place):
        return pltpu.make_async_remote_copy(
            src_ref=src, dst_ref=t_land.at[place],
            send_sem=t_send_sem.at[place], recv_sem=t_recv_sem.at[place],
            device_id={"atom": atom_at(by)}, device_id_type=MESH,
        )

    def feed():
        return pltpu.make_async_remote_copy(
            src_ref=t_self, dst_ref=fed, send_sem=feed_sem.at[0], recv_sem=feed_sem.at[1],
            device_id={"atom": atom_at(-ROW)}, device_id_type=MESH,
        )

    def t_down(d):
        t_copy(t_self, -d, SPAN + d).start()

    def ask(d):
        pl.semaphore_signal(ready.at[d - 1], inc=1, device_id={"atom": atom_at(d - ROW)}, device_id_type=MESH)

    feed().start()
    for d in range(1, SPAN + 1):
        pl.when(spot + d >= ROW)(functools.partial(ask, d))
    for d in range(1, SPAN + 1):
        t_copy(t_self, d, SPAN - d).start()
        pl.when(spot >= d)(functools.partial(t_down, d))

    where_to = lane16 - A_DEV * (iota((LM, LANES), 0) % 2)
    for place in range(PLACES):
        for a in range(A_DEV):
            pattern[place * A_DEV + a] = ones_where(where_to == place * LM + a).astype(BF16)
    pattern[PLACES * A_DEV] = jnp.zeros((LM, LANES), BF16)
    slot_out.wait()

    def hot(a, carry):
        for s in range(NB):
            q_buf[a, s * LM:(s + 1) * LM, :] = pattern[slot_of[a, s]]
        return carry

    lax.fori_loop(0, A_DEV, hot, 0)

    lax.fori_loop(EARLY, MIDDLE, turn, 0)

    def forward(d):
        pl.semaphore_wait(ready.at[d - 1], 1)
        t_copy(fed, ROW - d, SPAN + d).start()

    pl.when(spot < SPAN)(lambda: feed().wait_recv())
    for d in range(SPAN, 0, -1):
        pl.when(spot < d)(functools.partial(forward, d))
    lax.fori_loop(MIDDLE, A_DEV, turn, 0)


    t_land[SPAN] = t_self[...]
    for place in others:
        t_copy(t_self, place - SPAN, place).wait_recv()
    landed = t_land[...].reshape(PLACES * LM, LANES).astype(BF16)
    wide = jnp.dot(landed, spread_buf[...], preferred_element_type=F32).astype(BF16)
    for place in range(PLACES):
        for a in range(A_DEV):
            table[place * A_DEV + a] = wide[place * LM:(place + 1) * LM, a * LANES:(a + 1) * LANES]
    table[PLACES * A_DEV] = jnp.zeros((LM, LANES), BF16)

    keep = [ones_where(lane16 // LM == r).astype(BF16) for r in range(8)]

    def zone_blocks(a):
        for g in range(4):
            for h in range(2):
                for r in range(8):
                    s = g * 16 + h * 8 + r
                    bd_buf[a, g, r * LM:(r + 1) * LM, h * LANES:(h + 1) * LANES] = (
                        table[slot_of[a, s]] * keep[r]
                    )

    def zone(a):
        image = img_buf[a]
        parts = []
        for g in range(4):
            pair = jnp.concatenate(
                [image[:, 2 * g * LANES:(2 * g + 1) * LANES], image[:, (2 * g + 1) * LANES:(2 * g + 2) * LANES]],
                axis=0,
            )
            both = jnp.dot(pair, bd_buf[a, g], preferred_element_type=F32)
            parts.append(both[0:LM, 0:LANES])
            parts.append(both[LM:2 * LM, LANES:])
        parts[0] = parts[0] + first_buf[a]
        return jnp.concatenate([part.astype(BF16) for part in parts], axis=1)

    def sweep(a, flat):
        img_buf[a] = jnp.dot(flat, st_buf[a], preferred_element_type=F32).astype(BF16)

    pick = [ones_where((lane16 % LM) // 2 == h).astype(BF16) for h in range(8)]

    def zone_sum(a):
        image = img_buf[a]
        rows = jnp.concatenate([image * jnp.concatenate([pick[h]] * 8, axis=1) for h in range(8)], axis=0)
        return jnp.dot(rows, q_buf[a], preferred_element_type=F32)

    order = [(step, a) for step in range(SWEEPS - 1) for a in range(A_DEV)]
    zone_blocks(0)
    flat = zone(0)
    total = jnp.zeros((LANES, LANES), F32)
    for n, (step, a) in enumerate(order):
        ahead = None
        if n + 1 < len(order):
            if order[n + 1][0] == 0:
                zone_blocks(order[n + 1][1])
            ahead = zone(order[n + 1][1])
        if step == SWEEPS - 2 and a > 0:
            total = total + zone_sum(a - 1)
        sweep(a, flat)
        flat = ahead
    total = total + zone_sum(A_DEV - 1)
    g_send[...] = total.T

    def g_copy(place):
        return pltpu.make_async_remote_copy(
            src_ref=g_send.at[pl.ds(place * LM, LM)], dst_ref=g_land.at[2 * SPAN - place],
            send_sem=g_send_sem.at[place], recv_sem=g_recv_sem.at[2 * SPAN - place],
            device_id={"atom": atom_at(place - SPAN)}, device_id_type=MESH,
        )

    for place in others:
        g_copy(place).start()
    owned = g_send[SPAN * LM:(SPAN + 1) * LM, :]
    for place in others:
        g_copy(2 * SPAN - place).wait_recv()
        owned = owned + g_land[place]

    apart = ones_where(row // LM == lane // LM).astype(BF16)
    moved = [owned if d == 0 else pltpu.roll(owned, d * LM, 1) for d in range(8)]
    blocks = []
    for h in range(8):
        block = moved[(8 - h) % 8]
        for x in range(1, 8):
            block = jnp.where(lane16 // LM == x, moved[(x - h) % 8], block)
        blocks.append(block)
    owned_rows = jnp.concatenate(blocks, axis=0)
    high = owned_rows.astype(BF16)
    low = (owned_rows - high.astype(F32)).astype(BF16)
    received = jnp.dot(tbx_buf[...], jnp.concatenate([high, low], axis=0), preferred_element_type=F32)
    received_b = (received + t_tiled[...]).astype(BF16) * apart
    rad_in.wait()
    w_in.wait()
    radial = rad_ref[...]
    chunk = radial.shape[1] // n_energy

    def p_copy(by):
        return pltpu.make_async_remote_copy(
            src_ref=p_send.at[by], dst_ref=p_land.at[by - 1],
            send_sem=p_send_sem.at[by - 1], recv_sem=p_recv_sem.at[by - 1],
            device_id={"energy": energy_at(by)}, device_id_type=MESH,
        )

    for by in sorted(range(n_energy), key=lambda d: -min(d, n_energy - d)):
        part = rad_ref[:, pl.ds(pl.multiple_of(energy_at(by) * chunk, chunk), chunk)]
        turned = jnp.dot(received_b, part, preferred_element_type=F32)
        product = part.astype(F32) * turned
        p_send[by] = product.reshape(A_DEV, LM, chunk).sum(axis=1) * w_ref[0]
        if by:
            p_copy(by).start()
    density = p_send[0]
    for by in range(1, n_energy):
        p_copy(by).wait_recv()
        density = density + p_land[by - 1]
    out_ref[...] = density
    pl.when(spot >= SPAN)(lambda: feed().wait_recv())
    feed().wait_send()
    for place in others:
        t_copy(t_self, place - SPAN, place).wait_send()
        g_copy(place).wait_send()
    for by in range(1, n_energy):
        p_copy(by).wait_send()


def shards(n_atom, n_energy, t_matrix, structure, radial, weights, neighbours, live):
    r = radial.shape[-1]
    vmem = pl.BlockSpec(memory_space=pltpu.VMEM)
    hbm = pl.BlockSpec(memory_space=pl.ANY)
    return pl.pallas_call(
        functools.partial(kernel, n_atom, n_energy),
        out_shape=pltpu.VMEM((A_DEV, r // n_energy), F32),
        in_specs=[hbm] * 6,
        out_specs=vmem,
        scratch_shapes=[
            pltpu.VMEM((A_DEV * LM, LM), F32),
            pltpu.VMEM((A_DEV * LM, r), BF16),
            pltpu.SMEM((1,), F32),
            pltpu.VMEM((A_DEV, NB), jnp.int32),
            pltpu.VMEM((A_DEV, NB), jnp.int32),
            pltpu.VMEM((A_DEV, NB), jnp.int32),
            pltpu.VMEM((PLACES * A_DEV + 8, LM, LANES), BF16),
            pltpu.VMEM((A_DEV, SIZE, SIZE), BF16),
            pltpu.VMEM((A_DEV, SIZE, SIZE), BF16),
            pltpu.VMEM((A_DEV, SIZE, LANES), BF16),
            pltpu.VMEM((A_DEV, 4, LANES, TILE), BF16),
            pltpu.VMEM((PLACES * A_DEV + 8, LM, LANES), BF16),
            pltpu.VMEM((LM, LANES), F32),
            pltpu.VMEM((PLACES, LM, LANES), F32),
            pltpu.VMEM((A_DEV, LM, LANES), F32),
            pltpu.VMEM((A_DEV, LM, SIZE), BF16),
            pltpu.VMEM((LANES, A_DEV * LANES), BF16),
            pltpu.VMEM((LANES, 2 * LANES), BF16),
            pltpu.VMEM((LANES, LANES), F32),
            pltpu.VMEM((LANES, LANES), F32),
            pltpu.VMEM((PLACES, LM, LANES), F32),
            pltpu.VMEM((n_energy, A_DEV, r // n_energy), F32),
            pltpu.VMEM((n_energy - 1, A_DEV, r // n_energy), F32),
            pltpu.SMEM((A_DEV, NB), jnp.int32),
            pltpu.VMEM((TILE, TILE), BF16),
            pltpu.VMEM((LM, LANES), F32),
            pltpu.SemaphoreType.DMA((2,)),
            pltpu.SemaphoreType.REGULAR((SPAN,)),
            pltpu.SemaphoreType.DMA((6,)),
            pltpu.SemaphoreType.DMA((A_DEV,)),
            pltpu.SemaphoreType.DMA((PLACES,)),
            pltpu.SemaphoreType.DMA((PLACES,)),
            pltpu.SemaphoreType.DMA((PLACES,)),
            pltpu.SemaphoreType.DMA((PLACES,)),
            pltpu.SemaphoreType.DMA((n_energy - 1,)),
            pltpu.SemaphoreType.DMA((n_energy - 1,)),
        ],
        compiler_params=pltpu.CompilerParams(
            collective_id=0, has_side_effects=True, vmem_limit_bytes=60 * 1024 * 1024
        ),
    )(
        t_matrix.reshape(A_DEV * LM, LM),
        radial.reshape(A_DEV * LM, r),
        weights,
        neighbours,
        live,
        structure.reshape(A_DEV, SIZE, SIZE),
    )


def solution(mesh):
    in_specs = (
        P("energy", "atom", None, None),
        P("energy", "atom", None, None),
        P("energy", "atom", None, None),
        P("energy"),
        P("atom", None),
        P("atom", None),
    )
    body = functools.partial(shards, mesh.shape["atom"], mesh.shape["energy"])
    return jax.shard_map(body, mesh=mesh, in_specs=in_specs, out_specs=P("atom", "energy"), check_vma=False)
```
